32 devices in a mesh: lat: 4 (over y, x), lon: 4 (over z), lev: 2 (over core).
Axes of the slice: x: 2, y: 2, z: 4, core: 2. Of those that a mesh axis runs over, the one named last changes fastest.
Arguments:
- field_values: float32 [16, 256, 192, 128], P('lat', 'lon', 'lev'), may hold values from 0.2 to 1.8
- crowding: float32 [16, 256, 192, 128], P('lat', 'lon', 'lev'), may hold values from 0.5 to 2
Outputs:
- field_values_end: float32 [16, 256, 192, 128], P('lat', 'lon', 'lev')
The draws below stay inside these ranges and needn't reach their ends.
All inputs are finite; a program needn't handle non-finite values.
Results may differ from the reference program's by a relative error of at most 0.00002.
Values sent between devices are 32-bit elements; how exact they have to be, the bound alone decides.
A program may use at most 384 MiB of HBM per device.

```python
import jax
import jax.numpy as jnp
from jax import lax

GRID_J = 16
GRID_I = 256
GRID_K = 192
LEVELS = 128
STEPS = 3


def level_of(stream_key, shape, pieces, least, top_value):
    def one(axis_at, shards_of):
        heights = jax.random.uniform(jax.random.fold_in(jax.random.fold_in(stream_key, 6), axis_at), (shards_of,), jnp.float32, least / len(pieces), top_value / len(pieces))
        return jnp.repeat(jnp.exp(heights), shape[axis_at] // shards_of).reshape((-1,) + (1,) * (len(shape) - axis_at - 1))

    level = one(*pieces[0])
    for cut in pieces[1:]:
        level = level * one(*cut)
    return level


def setup_inputs(seed: int = 0) -> dict:
    arg_keys = jax.random.split(jax.random.key(seed), 3)
    field_values = jnp.clip(0.2 + 1.5999999 * jax.random.uniform(arg_keys[0], (GRID_J, GRID_I, GRID_K, LEVELS), jnp.float32) ** level_of(arg_keys[0], (GRID_J, GRID_I, GRID_K, LEVELS), ((0, 4), (1, 4), (2, 2)), -0.2, 0.2), 0.2, 1.8)
    crowding = jnp.clip(0.5 + 1.5 * jax.random.uniform(arg_keys[1], (GRID_J, GRID_I, GRID_K, LEVELS), jnp.float32) ** level_of(arg_keys[1], (GRID_J, GRID_I, GRID_K, LEVELS), ((0, 4), (1, 4), (2, 2)), -0.2, 0.2), 0.5, 2.0)
    return {"field_values": field_values, "crowding": crowding}


def without_rim(values, dims):
    for dim in dims:
        values = lax.slice_in_dim(values, 1, values.shape[dim] - 1, axis=dim)
    return values


def shifted_cells(values, dim, start, dims):
    others = [other for other in dims if other != dim]
    values = without_rim(values, others)
    return lax.slice_in_dim(values, start, start + values.shape[dim] - 2, axis=dim)


def march_step(padded, crowding):
    middle = without_rim(padded, (0, 1, 2))
    lower = [shifted_cells(padded, dim, 0, (0, 1, 2)) for dim in (0, 1, 2)]
    upper = [shifted_cells(padded, dim, 2, (0, 1, 2)) for dim in (0, 1, 2)]
    spread = lower[0] + upper[0] + lower[1] + upper[1] + lower[2] + upper[2] - 6.0 * middle
    return middle + 0.1 * spread + 0.2 * middle * (1.0 - middle * crowding)


def reference(field_values, crowding):
    for step in range(STEPS):
        field_values = march_step(jnp.pad(field_values, ((1, 1), (1, 1), (1, 1), (0, 0)), mode="wrap"), crowding)
    return field_values
```

```python
import functools
import math

import jax
import jax.numpy as jnp
from jax import lax
from jax.experimental import pallas as pl
from jax.experimental.pallas import tpu as pltpu
from jax.sharding import PartitionSpec as P

STEPS = 3
CHUNK_ROWS = 8
MESH = pl.DeviceIdType.MESH
AXES = ("lat", "lon", "lev")


def march_kernel(sizes, shape, rows, f_in, c_in, out, even, odd, crowd, jh, kh, kf,
                 load_sems, j_send, j_recv, i_send, i_recv, k_send, k_recv, out_sems):
    J, I, K, L = shape
    chunks = I // rows
    near = {}
    for axis, count in zip(AXES, sizes):
        me = lax.axis_index(axis)
        near[axis] = (lax.rem(me + count - 1, count), lax.rem(me + 1, count))

    barrier = pltpu.get_barrier_semaphore()
    for axis in AXES:
        for target in near[axis]:
            pl.semaphore_signal(barrier, inc=1, device_id={axis: target}, device_id_type=MESH)
    pl.semaphore_wait(barrier, 2 * len(AXES))

    fields = (even, odd)

    def remote(source, target, send, recv, axis, side):
        return pltpu.make_async_remote_copy(
            src_ref=source, dst_ref=target, send_sem=send, recv_sem=recv,
            device_id={axis: near[axis][side]}, device_id_type=MESH)

    def j_copy(step, side, chunk):
        j = (J - 1) * side
        if step == 0:
            source = f_in.at[j, pl.ds(chunk * rows, rows)]
        else:
            source = fields[step % 2].at[j, pl.ds(1 + chunk * rows, rows)]
        return remote(source, jh.at[step, 1 - side, pl.ds(chunk * rows, rows)],
                      j_send.at[step, side, chunk], j_recv.at[step, 1 - side, chunk], "lat", side)

    def i_copy(step, side):
        if step == 0:
            source = f_in.at[:, (I - 1) * side]
        else:
            source = fields[step % 2].at[:, 1 + (I - 1) * side]
        return remote(source, fields[step % 2].at[:, (I + 1) * (1 - side)],
                      i_send.at[step, side], i_recv.at[step, 1 - side], "lon", side)

    def k_copy(step, side):
        return remote(kf.at[step, side], kh.at[step, 1 - side],
                      k_send.at[step, side], k_recv.at[step, 1 - side], "lev", side)

    @pl.loop(0, chunks)
    def _(chunk):
        for side in (0, 1):
            j_copy(0, side, chunk).start()

    for side in (0, 1):
        i_copy(0, side).start()
    load_f = pltpu.make_async_copy(f_in, even.at[:, pl.ds(1, I)], load_sems.at[0])
    load_c = pltpu.make_async_copy(c_in, crowd, load_sems.at[1])
    load_f.start()
    load_c.start()
    load_f.wait()

    @pl.loop(0, I)
    def _(i):
        for j in range(J):
            kf[0, 0, j, pl.ds(i, 1), :] = even[j, i + 1, 0:1, :]
            kf[0, 1, j, pl.ds(i, 1), :] = even[j, i + 1, K - 1:K, :]

    load_c.wait()
    for side in (0, 1):
        k_copy(0, side).start()

    def out_copy(chunk):
        here = pl.ds(chunk * rows, rows)
        return pltpu.make_async_copy(
            fields[STEPS % 2].at[:, pl.ds(1 + chunk * rows, rows)], out.at[:, here],
            out_sems.at[chunk])

    at_k = lax.broadcasted_iota(jnp.int32, (K, L), 0)

    for step in range(STEPS):
        source, target = fields[step % 2], fields[(step + 1) % 2]
        last = step == STEPS - 1
        for side in (0, 1):
            i_copy(step, side).wait_recv()
            k_copy(step, side).wait_recv()
            if step >= 1:
                i_copy(step - 1, side).wait_send()

        def send_on(chunk):
            if last:
                out_copy(chunk).start()
            else:
                for side in (0, 1):
                    j_copy(step + 1, side, chunk).start()

        @pl.loop(0, chunks)
        def _(chunk):
            for side in (0, 1):
                j_copy(step, side, chunk).wait_recv()
                if step >= 1:
                    j_copy(step - 1, side, chunk).wait_send()

            @pl.loop(0, rows)
            def _(row):
                i = chunk * rows + row
                for j in range(J):
                    middle = source[j, i + 1]
                    below = jh[step, 0, i] if j == 0 else source[j - 1, i + 1]
                    above = jh[step, 1, i] if j == J - 1 else source[j + 1, i + 1]
                    total = below + above + source[j, i] + source[j, i + 2]
                    total += jnp.where(at_k == 0, kh[step, 0, j, pl.ds(i, 1), :],
                                       pltpu.roll(middle, 1, 0))
                    total += jnp.where(at_k == K - 1, kh[step, 1, j, pl.ds(i, 1), :],
                                       pltpu.roll(middle, K - 1, 0))
                    new = middle * (0.6 - 0.2 * (middle * crowd[j, i])) + 0.1 * total
                    target[j, i + 1] = new
                    if not last:
                        kf[step + 1, 0, j, pl.ds(i, 1), :] = new[0:1]
                        kf[step + 1, 1, j, pl.ds(i, 1), :] = new[K - 1:K]

            @pl.when(chunk > 0)
            def _():
                send_on(chunk - 1)

        send_on(chunks - 1)
        if not last:
            for side in (0, 1):
                i_copy(step + 1, side).start()
                k_copy(step + 1, side).start()

    for side in (0, 1):
        i_copy(STEPS - 1, side).wait_send()
        for step in range(STEPS):
            k_copy(step, side).wait_send()

    @pl.loop(0, chunks)
    def _(chunk):
        for side in (0, 1):
            j_copy(STEPS - 1, side, chunk).wait_send()
        out_copy(chunk).wait()


def local(sizes, field_values, crowding):
    J, I, K, L = shape = field_values.shape
    rows = math.gcd(I, CHUNK_ROWS)
    chunks = I // rows
    dtype = field_values.dtype
    DMA = pltpu.SemaphoreType.DMA
    return pl.pallas_call(
        functools.partial(march_kernel, sizes, shape, rows),
        out_shape=jax.ShapeDtypeStruct(shape, dtype),
        in_specs=[pl.BlockSpec(memory_space=pl.ANY)] * 2,
        out_specs=pl.BlockSpec(memory_space=pl.ANY),
        scratch_shapes=[
            pltpu.VMEM((J, I + 2, K, L), dtype),
            pltpu.VMEM((J, I + 2, K, L), dtype),
            pltpu.VMEM(shape, dtype),
            pltpu.VMEM((STEPS, 2, I, K, L), dtype),
            pltpu.VMEM((STEPS, 2, J, I, L), dtype),
            pltpu.VMEM((STEPS, 2, J, I, L), dtype),
            DMA((2,)),
            DMA((STEPS, 2, chunks)),
            DMA((STEPS, 2, chunks)),
            DMA((STEPS, 2)),
            DMA((STEPS, 2)),
            DMA((STEPS, 2)),
            DMA((STEPS, 2)),
            DMA((chunks,)),
        ],
        compiler_params=pltpu.CompilerParams(
            collective_id=0, has_side_effects=True, vmem_limit_bytes=67043328),
    )(field_values, crowding)


def solution(mesh):
    spec = P("lat", "lon", "lev", None)
    sizes = tuple(mesh.shape[axis] for axis in AXES)
    return jax.shard_map(
        functools.partial(local, sizes), mesh=mesh, in_specs=(spec, spec), out_specs=spec,
        check_vma=False,
    )
```

```python
import functools
import math

import jax
import jax.numpy as jnp
from jax import lax
from jax.experimental import pallas as pl
from jax.experimental.pallas import tpu as pltpu
from jax.sharding import PartitionSpec as P

STEPS = 3
CHUNK_ROWS = 8
WINDOW = 3
MESH = pl.DeviceIdType.MESH
AXES = ("lat", "lon", "lev")


def march_kernel(sizes, shape, rows, f_in, c_in, odd, even, crowd, jh, kh, kf,
                 load_sems, j_send, j_recv, i_send, i_recv, k_send, k_recv):
    J, I, K, L = shape
    chunks = I // rows
    near = {}
    for axis, count in zip(AXES, sizes):
        me = lax.axis_index(axis)
        near[axis] = (lax.rem(me + count - 1, count), lax.rem(me + 1, count))

    barrier = pltpu.get_barrier_semaphore()
    for axis in AXES:
        for target in near[axis]:
            pl.semaphore_signal(barrier, inc=1, device_id={axis: target}, device_id_type=MESH)
    pl.semaphore_wait(barrier, 2 * len(AXES))

    fields = (even, odd)

    def remote(source, target, send, recv, axis, side):
        return pltpu.make_async_remote_copy(
            src_ref=source, dst_ref=target, send_sem=send, recv_sem=recv,
            device_id={axis: near[axis][side]}, device_id_type=MESH)

    def j_copy(step, side, chunk):
        j = (J - 1) * side
        if step == 0:
            source = f_in.at[j, pl.ds(chunk * rows, rows)]
        else:
            source = fields[step % 2].at[j, pl.ds(1 + chunk * rows, rows)]
        return remote(source, jh.at[step, 1 - side, pl.ds(chunk * rows, rows)],
                      j_send.at[step, side, chunk], j_recv.at[step, 1 - side, chunk], "lat", side)

    def i_copy(step, side):
        if step == 0:
            source = f_in.at[:, (I - 1) * side]
        else:
            source = fields[step % 2].at[:, 1 + (I - 1) * side]
        return remote(source, fields[step % 2].at[:, (I + 1) * (1 - side)],
                      i_send.at[step, side], i_recv.at[step, 1 - side], "lon", side)

    def k_copy(step, side):
        return remote(kf.at[step, side], kh.at[step, 1 - side],
                      k_send.at[step, side], k_recv.at[step, 1 - side], "lev", side)

    window = min(WINDOW, chunks - 1)

    @pl.loop(0, window)
    def _(chunk):
        for side in (0, 1):
            j_copy(0, side, chunk).start()

    for side in (0, 1):
        i_copy(0, side).start()
    load_f = pltpu.make_async_copy(f_in, even.at[:, pl.ds(1, I)], load_sems.at[0])
    load_c = pltpu.make_async_copy(c_in, crowd, load_sems.at[1])
    load_f.start()
    load_c.start()
    load_f.wait()

    @pl.loop(0, I)
    def _(i):
        for j in range(J):
            kf[0, 0, j, pl.ds(i, 1), :] = even[j, i + 1, 0:1, :]
            kf[0, 1, j, pl.ds(i, 1), :] = even[j, i + 1, K - 1:K, :]

    load_c.wait()
    for side in (0, 1):
        k_copy(0, side).start()

    at_k = lax.broadcasted_iota(jnp.int32, (K, L), 0)

    for step in range(STEPS):
        source, target = fields[step % 2], fields[(step + 1) % 2]
        last = step == STEPS - 1
        for side in (0, 1):
            i_copy(step, side).wait_recv()
            k_copy(step, side).wait_recv()
            if step >= 1:
                i_copy(step - 1, side).wait_send()

        @pl.loop(0, chunks)
        def _(chunk):
            for side in (0, 1):
                j_copy(step, side, chunk).wait_recv()
                j_copy(step, side, chunk).wait_send()

            @pl.when(chunk + window < chunks)
            def _():
                for side in (0, 1):
                    j_copy(step, side, chunk + window).start()

            if not last:
                @pl.when(chunk + window >= chunks)
                def _():
                    for side in (0, 1):
                        j_copy(step + 1, side, chunk + window - chunks).start()

            @pl.loop(0, rows)
            def _(row):
                i = chunk * rows + row
                for j in range(J):
                    middle = source[j, i + 1]
                    below = jh[step, 0, i] if j == 0 else source[j - 1, i + 1]
                    above = jh[step, 1, i] if j == J - 1 else source[j + 1, i + 1]
                    total = below + above + source[j, i] + source[j, i + 2]
                    total += jnp.where(at_k == 0, kh[step, 0, j, pl.ds(i, 1), :],
                                       pltpu.roll(middle, 1, 0))
                    total += jnp.where(at_k == K - 1, kh[step, 1, j, pl.ds(i, 1), :],
                                       pltpu.roll(middle, K - 1, 0))
                    new = middle * (0.6 - 0.2 * (middle * crowd[j, i])) + 0.1 * total
                    target[j, i + 1] = new
                    if not last:
                        kf[step + 1, 0, j, pl.ds(i, 1), :] = new[0:1]
                        kf[step + 1, 1, j, pl.ds(i, 1), :] = new[K - 1:K]

        if not last:
            for side in (0, 1):
                i_copy(step + 1, side).start()
                k_copy(step + 1, side).start()

    for side in (0, 1):
        i_copy(STEPS - 1, side).wait_send()
        for step in range(STEPS):
            k_copy(step, side).wait_send()


def write_kernel(shape, held, out, sems):
    J, I = shape[:2]
    copies = [pltpu.make_async_copy(held.at[j, pl.ds(1, I)], out.at[j], sems.at[j])
              for j in range(J)]
    for copy in copies:
        copy.start()
    for copy in copies:
        copy.wait()


def local(sizes, field_values, crowding):
    J, I, K, L = shape = field_values.shape
    rows = math.gcd(I, CHUNK_ROWS)
    chunks = I // rows
    dtype = field_values.dtype
    DMA = pltpu.SemaphoreType.DMA
    marched = pl.pallas_call(
        functools.partial(march_kernel, sizes, shape, rows),
        out_shape=pltpu.VMEM((J, I + 2, K, L), dtype),
        in_specs=[pl.BlockSpec(memory_space=pl.ANY)] * 2,
        out_specs=pl.BlockSpec(memory_space=pltpu.VMEM),
        scratch_shapes=[
            pltpu.VMEM((J, I + 2, K, L), dtype),
            pltpu.VMEM(shape, dtype),
            pltpu.VMEM((STEPS, 2, I, K, L), dtype),
            pltpu.VMEM((STEPS, 2, J, I, L), dtype),
            pltpu.VMEM((STEPS, 2, J, I, L), dtype),
            DMA((2,)),
            DMA((STEPS, 2, chunks)),
            DMA((STEPS, 2, chunks)),
            DMA((STEPS, 2)),
            DMA((STEPS, 2)),
            DMA((STEPS, 2)),
            DMA((STEPS, 2)),
        ],
        compiler_params=pltpu.CompilerParams(
            collective_id=0, has_side_effects=True, vmem_limit_bytes=50 * 1024 * 1024),
    )(field_values, crowding)
    return pl.pallas_call(
        functools.partial(write_kernel, shape),
        out_shape=jax.ShapeDtypeStruct(shape, dtype),
        in_specs=[pl.BlockSpec(memory_space=pltpu.VMEM)],
        out_specs=pl.BlockSpec(memory_space=pl.ANY),
        scratch_shapes=[DMA((J,))],
        compiler_params=pltpu.CompilerParams(vmem_limit_bytes=1024 * 1024),
    )(pltpu.with_memory_space_constraint(marched, pltpu.VMEM))


def solution(mesh):
    spec = P("lat", "lon", "lev", None)
    sizes = tuple(mesh.shape[axis] for axis in AXES)
    return jax.shard_map(
        functools.partial(local, sizes), mesh=mesh, in_specs=(spec, spec), out_specs=spec,
        check_vma=False,
    )
```
